256 devices in a mesh: dp: 16 (over z_lo, y), mp: 16 (over x, z_hi, core).
Axes of the slice: x: 4, y: 4, z: 8 (z_hi: 2, z_lo: 4; z = z_hi * 4 + z_lo), core: 2. Of those that a mesh axis runs over, the one named last changes fastest.
Arguments:
- image_tokens: bfloat16 [16, 192, 3072], P('dp'), may hold values from -6 to 6
- text_tokens: bfloat16 [16, 64, 3072], P('dp'), may hold values from -6 to 6
- null_prompt: bfloat16 [64, 3072], replicated, may hold values from -6 to 6
- drop_flags: int32 [16], P('dp'), may hold values 0 or 1
- time_index: int32 [16], P('dp'), may hold values from 0 to 31
- modulation: float32 [32, 3, 3072], replicated, may hold values from -3 to 3
- w_up: bfloat16 [3072, 12288], P('dp', 'mp'), may hold values from -0.109375 to 0.109375
- w_down: bfloat16 [12288, 3072], P('mp', 'dp'), may hold values from -0.0546875 to 0.0546875
- d_output: bfloat16 [16, 256, 3072], P('dp'), may hold values from -6 to 6
Outputs:
- block_out: bfloat16 [16, 256, 3072], P('dp')
- d_tokens: bfloat16 [16, 256, 3072], P('dp')
- grad_up: float32 [3072, 12288], P('dp', 'mp')
- grad_down: float32 [12288, 3072], P('mp', 'dp')
- grad_null: float32 [64, 3072], replicated
The draws below stay inside these ranges and needn't reach their ends.
All inputs are finite; a program needn't handle non-finite values. No bound on the sum of `drop_flags` on one device may be relied on, other than what follows from the above.
Results may differ from the reference program's by a relative error of at most 0.017.
Values may be sent and summed in bfloat16 or wider, within the bound.
A program may use at most 128 MiB of HBM per device.

```python
import jax
import jax.numpy as jnp
from jax import lax

D = 3072
FF = 12288
L_IMG = 192
L_TXT = 64
NT = 32
B = 16
L = 256
N_MP = 16


def touch_ends(values, stream_key, low, largest):
    extent = values.shape
    place = [jax.random.randint(jax.random.fold_in(stream_key, axis), (), 0, extent[axis]) for axis in range(len(extent))]
    values = values.at[tuple(place)].set(low)
    longest = extent.index(max(extent))
    place[longest] = (place[longest] + 1) % extent[longest]
    return values.at[tuple(place)].set(largest)


def block_levels(key, shape, pieces, low, largest):
    gain = 1.0
    for axis_at, shards_of in pieces:
        heights = jax.random.uniform(jax.random.fold_in(jax.random.fold_in(key, 6), axis_at), (shards_of,), jnp.float32, low / len(pieces), largest / len(pieces))
        gain = gain * jnp.repeat(jnp.exp(heights), shape[axis_at] // shards_of).reshape((-1,) + (1,) * (len(shape) - 1 - axis_at))
    return gain


def gaussian(rng, dims, scale, most, shards=(), held_as=jnp.bfloat16):
    result = jax.random.normal(rng, dims, jnp.float32) * scale
    if len(shards) > 0:
        result = block_levels(rng, dims, shards, -0.22, 0.18) * result
    return jnp.clip(result, min=-most, max=most).astype(held_as)


def setup_inputs(seed: int = 0) -> dict:
    key_list = jax.random.split(jax.random.key(seed), 10)
    return {
        "image_tokens": gaussian(key_list[0], (B, L_IMG, D), 1.0, 6.0, ((0, 16),)),
        "text_tokens": gaussian(key_list[1], (B, L_TXT, D), 1.0, 6.0, ((0, 16),)),
        "null_prompt": gaussian(key_list[2], (L_TXT, D), 1.0, 6.0),
        "drop_flags": touch_ends((jax.random.randint(key_list[3], (B,), 0, 2) < 1).astype(jnp.int32), jax.random.fold_in(key_list[3], 1), 0, 1),
        "time_index": touch_ends(jax.random.randint(key_list[4], (B,), 0, NT), jax.random.fold_in(key_list[4], 1), 0, NT - 1).astype(jnp.int32),
        "modulation": gaussian(key_list[5], (NT, 3, D), 0.5, 3.0, (), jnp.float32),
        "w_up": gaussian(key_list[6], (D, FF), D ** -0.5, 0.109375, ((0, 16), (1, 16))),
        "w_down": gaussian(key_list[7], (FF, D), FF ** -0.5, 0.0546875, ((0, 16), (1, 16))),
        "d_output": gaussian(key_list[8], (B, L, D), 1.0, 6.0, ((0, 16),)),
    }


EPS = 1e-06

def gelu_tanh(values):
    return jax.nn.gelu(values, approximate=True)

def reference(image_tokens, text_tokens, null_prompt, drop_flags, time_index, modulation, w_up, w_down, d_output):
    dropped = drop_flags == 1
    text_in = jnp.where(dropped[:, None, None], null_prompt[None], text_tokens)
    joined = jnp.concatenate([text_in, image_tokens], axis=1)
    levels = jnp.arange(modulation.shape[0], dtype=jnp.int32)
    indicator_matrix = (time_index[:, None] == levels[None, :]).astype(jnp.float32)
    modulation_vectors = jnp.einsum('yi,imr->ymr', indicator_matrix, modulation.astype(jnp.float32), precision=lax.Precision.HIGHEST)
    shift_modulation = modulation_vectors[:, 0][:, None]
    scale_mod = modulation_vectors[:, 1][:, None]
    gate_mod = modulation_vectors[:, 2][:, None]
    batch, length, width = joined.shape
    joined32 = joined.astype(jnp.float32)
    centred = joined32 - lax.optimization_barrier(jnp.mean(joined32, axis=-1, keepdims=True))
    inv_std = lax.rsqrt(lax.optimization_barrier(jnp.mean(centred * centred, axis=-1, keepdims=True)) + EPS)
    normed = centred * inv_std
    mod_in = (normed * (1.0 + scale_mod) + shift_modulation).astype(jnp.bfloat16)
    flat_in = mod_in.reshape(batch * length, width)
    preactivation_rows = jnp.dot(flat_in, w_up, preferred_element_type=jnp.float32)
    hidden = gelu_tanh(preactivation_rows).astype(jnp.bfloat16)
    per_part = w_up.shape[1] // N_MP
    block_ids = jnp.arange(N_MP, dtype=jnp.int32)

    def add_branch(total, block_no):
        start = (block_no * per_part).astype(jnp.int32)
        cols = lax.dynamic_slice_in_dim(hidden, start, per_part, 1)
        rows_w = lax.dynamic_slice_in_dim(w_down, start, per_part, 0)
        part = jnp.dot(cols, rows_w, preferred_element_type=jnp.float32).astype(jnp.bfloat16)
        part = lax.optimization_barrier(part)
        return (total + part.astype(jnp.float32), None)
    branch, _ = lax.scan(add_branch, jnp.zeros((batch * length, width), jnp.float32), block_ids)
    branch = branch.reshape(batch, length, width)
    block_out = (joined32 + gate_mod * branch).astype(jnp.bfloat16)
    d_out32 = d_output.astype(jnp.float32)
    d_branch = (d_out32 * gate_mod).astype(jnp.bfloat16).reshape(batch * length, width)
    hidden_gradient = jnp.dot(d_branch, w_down.T, preferred_element_type=jnp.float32)
    _, gelu_back = jax.vjp(gelu_tanh, preactivation_rows)
    d_pre = gelu_back(hidden_gradient)[0].astype(jnp.bfloat16)
    grad_down = jnp.dot(hidden.T, d_branch, preferred_element_type=jnp.float32)
    grad_up = jnp.dot(flat_in.T, d_pre, preferred_element_type=jnp.float32)

    def add_input(total, block_no):
        start = (block_no * per_part).astype(jnp.int32)
        cols = lax.dynamic_slice_in_dim(d_pre, start, per_part, 1)
        wcols = lax.dynamic_slice_in_dim(w_up, start, per_part, 1)
        part = jnp.dot(cols, wcols.T, preferred_element_type=jnp.float32).astype(jnp.bfloat16)
        part = lax.optimization_barrier(part)
        return (total + part.astype(jnp.float32), None)
    d_mod, _ = lax.scan(add_input, jnp.zeros((batch * length, width), jnp.float32), block_ids)
    d_normed = d_mod.reshape(batch, length, width) * (1.0 + scale_mod)
    d_full = d_out32 + inv_std * (d_normed - lax.optimization_barrier(jnp.mean(d_normed, axis=-1, keepdims=True)) - normed * lax.optimization_barrier(jnp.mean(d_normed * normed, axis=-1, keepdims=True)))
    grad_null = lax.optimization_barrier(jnp.sum(jnp.where(dropped[:, None, None], d_full[:, :L_TXT], jnp.float32(0.0)), axis=0))
    return (block_out, d_full.astype(jnp.bfloat16), grad_up, grad_down, grad_null)
```

```python
import functools

import jax
import jax.numpy as jnp
from jax import lax
from jax.experimental import pallas as pl
from jax.experimental.pallas import tpu as pltpu
from jax.sharding import Mesh
from jax.sharding import PartitionSpec as P

AXES = ("zl", "y", "x", "zh", "c")
MP = ("x", "zh", "c")
DP = ("zl", "y")
EPS = 1e-06
MESH = pl.DeviceIdType.MESH
BF = jnp.bfloat16
F32 = jnp.float32


def gelu_tanh(values):
    return jax.nn.gelu(values, approximate=True)


def remote(src, dst, ss, rs, **dev):
    return pltpu.make_async_remote_copy(
        src_ref=src, dst_ref=dst, send_sem=ss, recv_sem=rs, device_id=dev, device_id_type=MESH
    )


def meet(devices):
    barrier = pltpu.get_barrier_semaphore()
    for dev in devices:
        pl.semaphore_signal(barrier, inc=1, device_id=dev, device_id_type=MESH)
    pl.semaphore_wait(barrier, len(devices))


def along_z(zl, zh, dist):
    to = lax.rem(zh * 4 + zl + dist % 8, 8)
    return {"zl": lax.rem(to, 4), "zh": to // 4}


def gather_kernel(pk, ab, g, t, lsem, ws, wr, zs, zr, ys, yr, ps, pr, xs, xr, bs, br):
    zl, y, x, zh, c = (lax.axis_index(n) for n in AXES)
    meet(
        [{"y": lax.rem(y + d, 4)} for d in (1, 2, 3)]
        + [{"x": lax.rem(x + d, 4)} for d in (1, 3)]
        + [along_z(zl, zh, d) for d in (1, -1)]
        + [{"c": 1 - c}]
    )
    yp, yo, ym = lax.rem(y + 1, 4), lax.rem(y + 2, 4), lax.rem(y + 3, 4)
    xp, xm = lax.rem(x + 1, 4), lax.rem(x + 3, 4)
    qrt = ab.shape[1] // 4
    half = qrt // 2
    par = lax.rem(x, 2)
    peers = (ym, yp, yo)
    sent = []

    def rows(quarter, h, n=1):
        return pl.ds(pl.multiple_of(quarter * qrt + h * half, half), n * half)

    own_q = par * 2 + c
    x_q = (1 - par) * 2 + c
    sib_q = (par * 2 + (1 - c), (1 - par) * 2 + (1 - c))

    def w1(d):
        to = lax.rem(y + d, 4)
        return remote(pk.at[to], g.at[zl, y], ws.at[d - 1], wr.at[d - 1], y=to)

    for d in (1, 3, 2):
        w1(d).start()
        sent.append((None, w1(d)))
    locs = [pltpu.make_async_copy(pk.at[y], g.at[zl, y], lsem.at[0])]
    locs += [pltpu.make_async_copy(ab.at[a], t.at[a, y], lsem.at[1 + a]) for a in range(2)]
    for cp in locs:
        cp.start()

    for a in range(2):
        for way, to in ((0, yp), (1, ym)):
            cp = remote(
                ab.at[a, rows(own_q, 0, 2)],
                t.at[a, y, rows(own_q, 0, 2)],
                ys.at[a, way],
                yr.at[a, way],
                y=to,
            )
            cp.start()
            sent.append((None, cp))

    def zcopy(way, s, d):
        yd = lax.rem(y + 4 - d, 4)
        block = zl - s if way == 0 else zl + s
        src = pk.at[y] if (s == 0 and d == 0) else g.at[block, yd]
        to = zl + 1 if way == 0 else zl - 1
        return remote(src, g.at[block, yd], zs.at[way, s, d], zr.at[way, s, d], zl=to)

    def zsend(way, s, d):
        ok = (zl < 3) & (zl >= s) if way == 0 else (zl > 0) & (zl + s <= 3)

        @pl.when(ok)
        def _():
            zcopy(way, s, d).start()

        sent.append((ok, (way, s, d)))

    def ztick(s, d):
        for way in (0, 1):
            got = zl >= s if way == 0 else zl + s <= 3
            yd = lax.rem(y + 4 - d, 4)

            @pl.when(got)
            def _():
                block = zl - s if way == 0 else zl + s
                remote(
                    g.at[block, yd], g.at[block, yd], zs.at[way, s - 1, d], zr.at[way, s - 1, d], zl=zl
                ).wait_recv()

            if s <= 2:
                zsend(way, s, d)

    def wstep(d):
        if d:
            w1(d).wait_recv()
        for way in (0, 1):
            zsend(way, 0, d)

    wstep(0)
    wstep(1)
    wstep(3)

    def send_on(a, peer, h):
        src = t.at[a, peers[peer], rows(own_q, h)]
        for cp in (
            remote(src, src, xs.at[a, peer, h], xr.at[a, peer, h], x=(xp, xm)[h]),
            remote(src, src, bs.at[a, peer, h], br.at[a, peer, h], c=1 - c),
        ):
            cp.start()
            sent.append((None, cp))

    def direct(a, way):
        whole = t.at[a, peers[way], rows(own_q, 0, 2)]
        remote(whole, whole, ys.at[a, way], yr.at[a, way], y=y).wait_recv()
        part = t.at[a, peers[way], rows(own_q, way)]
        cp = remote(part, part, ps.at[a, way], pr.at[a, way], y=(yp, ym)[way])
        cp.start()
        sent.append((None, cp))
        for h in (0, 1):
            send_on(a, way, h)

    def relayed(a, h):
        part = t.at[a, yo, rows(own_q, h)]
        remote(part, part, ps.at[a, h], pr.at[a, h], y=y).wait_recv()
        send_on(a, 2, h)

    def from_x(a, peer):
        for h in (0, 1):
            part = t.at[a, peers[peer], rows(x_q, h)]
            remote(part, part, xs.at[a, peer, h], xr.at[a, peer, h], x=x).wait_recv()
            cp = remote(part, part, bs.at[a, peer, 2 + h], br.at[a, peer, 2 + h], c=1 - c)
            cp.start()
            sent.append((None, cp))

    ztick(1, 0)
    wstep(2)
    ztick(1, 1)
    direct(0, 1)
    ztick(1, 3)
    ztick(1, 2)
    direct(0, 0)
    ztick(2, 0)
    direct(1, 1)
    ztick(2, 1)
    relayed(0, 1)
    from_x(0, 1)
    direct(1, 0)
    ztick(2, 3)
    from_x(0, 0)
    ztick(2, 2)
    relayed(1, 1)
    relayed(0, 0)
    ztick(3, 0)
    from_x(1, 1)
    relayed(1, 0)
    ztick(3, 1)
    from_x(1, 0)
    from_x(0, 2)
    ztick(3, 3)
    ztick(3, 2)
    from_x(1, 2)
    for a in range(2):
        for peer in range(3):
            for kind in range(4):
                part = t.at[a, peers[peer], rows(sib_q[kind // 2], kind % 2)]
                remote(part, part, bs.at[a, peer, kind], br.at[a, peer, kind], c=c).wait_recv()
    for cp in locs:
        cp.wait()
    for ok, cp in sent:
        if ok is None:
            cp.wait_send()
        else:
            way, s, d = cp

            @pl.when(ok)
            def _():
                zcopy(way, s, d).wait_send()


def gather(pk, ab):
    n_tok, width = ab.shape[1:]
    hid, lanes = pk.shape[1:]
    dma = pltpu.SemaphoreType.DMA
    return pl.pallas_call(
        gather_kernel,
        out_shape=(
            jax.ShapeDtypeStruct((4, 4, hid, lanes), BF),
            jax.ShapeDtypeStruct((2, 4, n_tok, width), BF),
        ),
        in_specs=[pl.BlockSpec(memory_space=pltpu.VMEM)] * 2,
        out_specs=(pl.BlockSpec(memory_space=pl.ANY),) * 2,
        scratch_shapes=[
            dma((3,)),
            dma((3,)),
            dma((3,)),
            dma((2, 3, 4)),
            dma((2, 3, 4)),
            dma((2, 2)),
            dma((2, 2)),
            dma((2, 2)),
            dma((2, 2)),
            dma((2, 3, 2)),
            dma((2, 3, 2)),
            dma((2, 3, 4)),
            dma((2, 3, 4)),
        ],
        compiler_params=pltpu.CompilerParams(
            collective_id=1, has_side_effects=True, vmem_limit_bytes=60 * 2**20
        ),
        name="gather_all",
    )(pk, ab)


def reduce_kernel(
    pp, qq, jo, do, mods, flag,
    ob, gn, gr,
    R, X1, F1, X2, F2, RB, Z, O, FIN, ZR, ZL, YN, ZN, GN,
    lsem, cs, cr, e1s, e1r, e2s, e2r, hs, hr, hs2, hr2, zs, zr, ws, wr, ags, agr, ags2, agr2, abs_, abr,
    gys, gyr, gzs, gzr, gxs, gxr, gbs, gbr,
):
    zl, y, x, zh, c = (lax.axis_index(n) for n in AXES)
    meet(
        [{"y": lax.rem(y + d, 4)} for d in (1, 2, 3)]
        + [{"x": lax.rem(x + d, 4)} for d in (1, 2, 3)]
        + [along_z(zl, zh, d) for d in (1, -1, 2, -2, 3, -3)]
        + [{"c": 1 - c}]
    )
    xp, xo, xm = lax.rem(x + 1, 4), lax.rem(x + 2, 4), lax.rem(x + 3, 4)
    first = c == 0
    p1 = jnp.where(first, y, x)
    p2 = jnp.where(first, x, y)
    n_r, width = pp.shape[4:]
    step_r = 16
    blocks = n_r // step_r
    tail = []

    def start(cp, ok=None):
        cp.start()
        tail.append((ok, cp))

    def nb(stage, sign):
        s = sign % 4
        along_y = first if stage == 1 else c == 1
        return {
            "y": jnp.where(along_y, lax.rem(y + s, 4), y),
            "x": jnp.where(along_y, x, lax.rem(x + s, 4)),
        }

    def zpiece(way, k, p, from_input):
        buf = ZR if way == 0 else ZL
        src = qq.at[k, p] if from_input else buf.at[k, p]
        to = zl + 1 if way == 0 else zl - 1
        return remote(src, buf.at[k, p], zs.at[way, k, p], zr.at[way, k, p], zl=to)

    hid = qq.shape[2]

    def q_add(buf, k, p):
        def body(i, carry):
            r = pl.ds(pl.multiple_of(i * 48, 16), 48)
            buf[k, p, r, :] = (buf[k, p, r, :].astype(F32) + qq[k, p, r, :].astype(F32)).astype(BF)
            return carry

        lax.fori_loop(0, hid // 48, body, 0)

    zorder = [(s, p) for s in range(3) for p in range(4)]
    for s, p in zorder:

        @pl.when(zl == 0)
        def _():
            zpiece(0, 3 - s, p, True).start()

        @pl.when(zl == 3)
        def _():
            zpiece(1, s, p, True).start()

    def ztick(s, p):
        for way in (0, 1):
            k = 3 - s if way == 0 else s
            mid = (zl > 0) & (zl < k) if way == 0 else (zl < 3) & (zl > k)

            @pl.when(mid)
            def _():
                zpiece(way, k, p, False).wait_recv()
                q_add(ZR if way == 0 else ZL, k, p)
                zpiece(way, k, p, False).start()

    o_first = c == 1
    op1 = jnp.where(o_first, y, x)
    for d in (2, 1, 3, 0):
        for a in range(2):
            k = lax.rem(op1 + d, 4)
            for j in range(4):
                iy, ix = jnp.where(o_first, k, j), jnp.where(o_first, j, k)
                remote(
                    pp.at[a, iy, 1 - c, ix], R.at[a, k, j], cs.at[a, d], cr.at[a, d], c=1 - c
                ).start()

    def own_sum(a, d):
        k = lax.rem(p1 + d, 4)
        remote(R.at[a, k], R.at[a, k], cs.at[a, d], cr.at[a, d], c=c).wait_recv()

        def body(n, carry):
            j, r = n // blocks, lax.rem(n, blocks)
            iy, ix = jnp.where(first, k, j), jnp.where(first, j, k)
            rr = pl.ds(pl.multiple_of(r * step_r, step_r), step_r)
            R[a, k, j, rr, :] = (
                R[a, k, j, rr, :].astype(F32) + pp[a, iy, c, ix, rr, :].astype(F32)
            ).astype(BF)
            return carry

        lax.fori_loop(0, 4 * blocks, body, 0)

    def view(stage, a, d):
        if stage == 1:
            return R.at[a, lax.rem(p1 + d, 4)]
        return R.at[a, p1, lax.rem(p2 + d, 4)]

    def bufs(stage):
        return (X1, F1, e1s, e1r) if stage == 1 else (X2, F2, e2s, e2r)

    def add_to(dst, *srcs):
        if len(dst.shape) == 3:

            def body(n, carry):
                j, r = n // blocks, lax.rem(n, blocks)
                rr = pl.ds(pl.multiple_of(r * step_r, step_r), step_r)
                total = dst[j, rr, :].astype(F32)
                for s in srcs:
                    total = total + s[j, rr, :].astype(F32)
                dst[j, rr, :] = total.astype(BF)
                return carry

            lax.fori_loop(0, dst.shape[0] * blocks, body, 0)
        else:

            def body(r, carry):
                rr = pl.ds(pl.multiple_of(r * step_r, step_r), step_r)
                total = dst[rr, :].astype(F32)
                for s in srcs:
                    total = total + s[rr, :].astype(F32)
                dst[rr, :] = total.astype(BF)
                return carry

            lax.fori_loop(0, blocks, body, 0)

    def ring_first(stage, a):
        X, F, es, er = bufs(stage)
        sg = 1 if a == 0 else -1
        start(remote(view(stage, a, 2), X.at[a], es.at[a, 0], er.at[a, 0], **nb(stage, sg)))

    def ring_own(stage, a):
        X, F, es, er = bufs(stage)
        sg = 1 if a == 0 else -1
        start(remote(view(stage, a, -sg % 4), F.at[1, a], es.at[a, 1], er.at[a, 1], **nb(stage, -sg)))

    def ring_pass(stage, a):
        X, F, es, er = bufs(stage)
        sg = 1 if a == 0 else -1
        cp = remote(X.at[a], X.at[a], es.at[a, 0], er.at[a, 0], c=c)
        cp.wait_recv()
        mine = view(stage, a, sg % 4)
        add_to(mine, X.at[a])
        start(remote(mine, F.at[0, a], es.at[a, 2], er.at[a, 2], **nb(stage, sg)))

    def ring_last(stage, a):
        X, F, es, er = bufs(stage)
        remote(F.at[1, a], F.at[1, a], es.at[a, 1], er.at[a, 1], c=c).wait_recv()
        remote(F.at[0, a], F.at[0, a], es.at[a, 2], er.at[a, 2], c=c).wait_recv()
        add_to(view(stage, a, 0), F.at[0, a], F.at[1, a])

    own_sum(1, 2)
    ring_first(1, 1)
    own_sum(0, 2)
    ring_first(1, 0)
    ztick(0, 0)
    own_sum(0, 3)
    ring_own(1, 0)
    own_sum(1, 1)
    ring_own(1, 1)
    ztick(0, 1)
    own_sum(1, 3)
    own_sum(0, 1)
    own_sum(1, 0)
    own_sum(0, 0)
    ztick(0, 2)
    ring_pass(1, 1)
    ring_pass(1, 0)
    ztick(0, 3)
    for p in range(4):
        ztick(1, p)
    for a in (1, 0):
        ring_last(1, a)
        ring_first(2, a)
        ring_own(2, a)
    for a in (1, 0):
        ring_pass(2, a)

    hr_n = n_r // 2

    def half_rows(way):
        return pl.ds(way * hr_n, hr_n)

    def zh_send(a, way):
        mine = R.at[a, p1, p2, half_rows(way)]
        return remote(mine, RB.at[a, way], hs.at[a, way], hr.at[a, way], **along_z(zl, zh, (1, -1)[way]))

    def zh_pass(a, way):
        return remote(
            RB.at[a, way], Z.at[a, half_rows(way)], hs2.at[a, way], hr2.at[a, way], **along_z(zl, zh, (3, -3)[way])
        )

    for a in (1, 0):
        ring_last(2, a)
        for way in (0, 1):
            start(zh_send(a, way))

    def wcopy(d):
        to = lax.rem(y + d, 4)
        return remote(FIN.at[to], gr.at[y], ws.at[d], wr.at[d], y=to)

    def grad_final(d):
        p = lax.rem(y + d, 4)

        @pl.when(zl > 0)
        def _():
            remote(ZR.at[zl, p], ZR.at[zl, p], zs.at[0, zl, p], zr.at[0, zl, p], c=c).wait_recv()

        @pl.when(zl < 3)
        def _():
            remote(ZL.at[zl, p], ZL.at[zl, p], zs.at[1, zl, p], zr.at[1, zl, p], c=c).wait_recv()

        def body(i, carry):
            r = pl.ds(pl.multiple_of(i * 48, 16), 48)
            zero = jnp.zeros((48, qq.shape[3]), F32)
            total = qq[zl, p, r, :].astype(F32)
            total = total + jnp.where(zl > 0, ZR[zl, p, r, :].astype(F32), zero)
            total = total + jnp.where(zl < 3, ZL[zl, p, r, :].astype(F32), zero)
            FIN[p, r, :] = total.astype(BF)
            return carry

        lax.fori_loop(0, hid // 48, body, 0)
        if d:
            start(wcopy(d))

    for d in (2, 1, 3, 0):
        grad_final(d)
    loc_gr = pltpu.make_async_copy(FIN.at[y], gr.at[y], lsem.at[0])
    loc_gr.start()

    for a in (1, 0):
        for way in (0, 1):
            remote(RB.at[a, way], RB.at[a, way], hs.at[a, way], hr.at[a, way], c=c).wait_recv()
            start(zh_pass(a, way))

    blk = c * 4 + x
    row0 = blk * n_r
    n_text = YN.shape[1]

    def rows_done(a):
        for way in (0, 1):
            part = Z.at[a, half_rows(way)]
            remote(part, part, hs2.at[a, way], hr2.at[a, way], c=c).wait_recv()

        def body(r, carry):
            rr = pl.ds(pl.multiple_of(r * 16, 16), 16)
            at = pl.ds(pl.multiple_of(row0 + r * 16, 16), 16)
            total = R[a, p1, p2, rr, :].astype(F32) + Z[a, rr, :].astype(F32)
            tok = jo[at, :].astype(F32)
            if a == 0:
                O[0, rr, :] = (tok + mods[2:3, :] * total).astype(BF)
            else:
                cen = tok - jnp.mean(tok, axis=-1, keepdims=True)
                inv = lax.rsqrt(jnp.mean(cen * cen, axis=-1, keepdims=True) + EPS)
                normed = cen * inv
                dn = total * (1.0 + mods[1:2, :])
                full = do[at, :].astype(F32) + inv * (
                    dn
                    - jnp.mean(dn, axis=-1, keepdims=True)
                    - normed * jnp.mean(dn * normed, axis=-1, keepdims=True)
                )
                O[1, rr, :] = full.astype(BF)

                @pl.when(r == 0)
                def _():
                    YN[y] = jnp.where(flag[0:1, :] > 0.5, full[:n_text], 0.0).astype(BF)

            return carry

        lax.fori_loop(0, n_r // 16, body, 0)

    locs = [loc_gr]

    def gather_start(a):
        for way, to in ((0, xp), (1, xm)):
            start(remote(O.at[a], ob.at[a, blk], ags.at[a, way], agr.at[a, way], x=to))
        start(remote(O.at[a], ob.at[a, blk], abs_.at[a, 0], abr.at[a, 0], c=1 - c))
        cp = pltpu.make_async_copy(O.at[a], ob.at[a, blk], lsem.at[1 + a])
        cp.start()
        locs.append(cp)

    def gather_near(a):
        for way, frm in ((0, xm), (1, xp)):
            part = ob.at[a, c * 4 + frm]
            remote(part, part, ags.at[a, way], agr.at[a, way], x=x).wait_recv()
            if way == a:
                start(remote(part, part, ags2.at[a], agr2.at[a], x=(xp, xm)[way]))
            start(remote(part, part, abs_.at[a, 1 + way], abr.at[a, 1 + way], c=1 - c))

    def gather_far(a):
        part = ob.at[a, c * 4 + xo]
        remote(part, part, ags2.at[a], agr2.at[a], x=x).wait_recv()
        start(remote(part, part, abs_.at[a, 3], abr.at[a, 3], c=1 - c))

    def gy(d):
        return remote(YN.at[y], YN.at[y], gys.at[d], gyr.at[d], y=lax.rem(y + d, 4))

    def gz(d):
        return remote(ZN.at[zl], ZN.at[zl], gzs.at[d], gzr.at[d], zl=lax.rem(zl + d, 4))

    def gx(d):
        return remote(GN, gn.at[blk], gxs.at[d], gxr.at[d], x=lax.rem(x + d, 4))

    def sum_slots(src, dst):
        total = src[0].astype(F32)
        for i in range(1, 4):
            total = total + src[i].astype(F32)
        dst[...] = total.astype(BF)

    def got(buf, me, sems, semr):
        for d in (1, 3, 2):
            slot = buf.at[lax.rem(me + 4 - d, 4)]
            remote(slot, slot, sems.at[d], semr.at[d], c=c).wait_recv()

    rows_done(1)
    for d in (2, 1, 3):
        start(gy(d))
    gather_start(1)
    got(YN, y, gys, gyr)
    sum_slots(YN, ZN.at[zl])
    for d in (1, 2, 3):
        start(gz(d))
    rows_done(0)
    gather_start(0)
    gather_near(1)
    got(ZN, zl, gzs, gzr)
    sum_slots(ZN, GN)
    for d in (2, 1, 3):
        start(gx(d))
    start(remote(GN, gn.at[blk], gbs.at[0], gbr.at[0], c=1 - c))
    loc_gn = pltpu.make_async_copy(GN, gn.at[blk], lsem.at[3])
    loc_gn.start()
    locs.append(loc_gn)
    gather_far(1)
    gather_near(0)
    for d in (1, 3, 2):
        part = gn.at[c * 4 + lax.rem(x + 4 - d, 4)]
        remote(part, part, gxs.at[d], gxr.at[d], x=x).wait_recv()
        start(remote(part, part, gbs.at[d], gbr.at[d], c=1 - c))
    gather_far(0)
    for d in range(4):
        part = gn.at[(1 - c) * 4 + lax.rem(x + 4 - d, 4)]
        remote(part, part, gbs.at[d], gbr.at[d], c=c).wait_recv()

    for a in range(2):
        for i, frm in enumerate((x, xm, xp, xo)):
            part = ob.at[a, (1 - c) * 4 + frm]
            remote(part, part, abs_.at[a, i], abr.at[a, i], c=c).wait_recv()
    for d in (1, 2, 3):
        frm = gr.at[lax.rem(y + 4 - d, 4)]
        remote(frm, frm, ws.at[d], wr.at[d], y=y).wait_recv()
    for cp in locs:
        cp.wait()
    for _, cp in tail:
        cp.wait_send()
    for d in (2, 1, 3, 0):
        for a in range(2):
            remote(R.at[a, 0], R.at[a, 0], cs.at[a, d], cr.at[a, d], c=1 - c).wait_send()
    for s, p in zorder:
        for way in (0, 1):
            k = 3 - s if way == 0 else s
            did = zl < k if way == 0 else zl > k

            @pl.when(did)
            def _():
                zpiece(way, k, p, False).wait_send()


def reduce_all(pp, qq, jo, do, mods, flag):
    n_r, width = pp.shape[4:]
    hid, lanes = qq.shape[2:]
    dma = pltpu.SemaphoreType.DMA
    vm = pl.BlockSpec(memory_space=pltpu.VMEM)
    hbm = pl.BlockSpec(memory_space=pl.ANY)
    blk = (n_r, width)
    return pl.pallas_call(
        reduce_kernel,
        out_shape=(
            jax.ShapeDtypeStruct((2, 8, *blk), BF),
            jax.ShapeDtypeStruct((8, n_r // 4, width), BF),
            jax.ShapeDtypeStruct((4, hid, lanes), BF),
        ),
        in_specs=[vm] * 6,
        out_specs=(hbm,) * 3,
        scratch_shapes=[
            pltpu.VMEM((2, 4, 4, *blk), BF),
            pltpu.VMEM((2, 4, *blk), BF),
            pltpu.VMEM((2, 2, 4, *blk), BF),
            pltpu.VMEM((2, *blk), BF),
            pltpu.VMEM((2, 2, *blk), BF),
            pltpu.VMEM((2, 2, n_r // 2, width), BF),
            pltpu.VMEM((2, *blk), BF),
            pltpu.VMEM((2, *blk), BF),
            pltpu.VMEM((4, hid, lanes), BF),
            pltpu.VMEM((4, 4, hid, lanes), BF),
            pltpu.VMEM((4, 4, hid, lanes), BF),
            pltpu.VMEM((4, n_r // 4, width), BF),
            pltpu.VMEM((4, n_r // 4, width), BF),
            pltpu.VMEM((n_r // 4, width), BF),
            dma((4,)),
            dma((2, 4)),
            dma((2, 4)),
            dma((2, 3)),
            dma((2, 3)),
            dma((2, 3)),
            dma((2, 3)),
            dma((2, 2)),
            dma((2, 2)),
            dma((2, 2)),
            dma((2, 2)),
            dma((2, 4, 4)),
            dma((2, 4, 4)),
            dma((4,)),
            dma((4,)),
            dma((2, 2)),
            dma((2, 2)),
            dma((2,)),
            dma((2,)),
            dma((2, 4)),
            dma((2, 4)),
            dma((4,)),
            dma((4,)),
            dma((4,)),
            dma((4,)),
            dma((4,)),
            dma((4,)),
            dma((4,)),
            dma((4,)),
        ],
        compiler_params=pltpu.CompilerParams(
            collective_id=2, has_side_effects=True, vmem_limit_bytes=60 * 2**20
        ),
        name="reduce_all",
    )(pp, qq, jo, do, mods, flag)


def dot(left, right, dims):
    return lax.dot_general(left, right, (dims, ((), ())), preferred_element_type=F32)


def mlp_kernel(g, t, pp, qq, up, dn, gu, gd):
    m = pl.program_id(0)
    width = up.shape[1]
    hid, lanes = g.shape[1:]
    part = lanes // 2
    pairs = g.shape[0] // 2

    @pl.when(m == 0)
    def _():
        for j in range(pairs):
            at = slice(j * lanes, (j + 1) * lanes)
            up[:, at] = jnp.concatenate([g[2 * j, :, :part], g[2 * j + 1, :, :part]], axis=1)
            dn[:, at] = jnp.concatenate([g[2 * j, :, part:], g[2 * j + 1, :, part:]], axis=1)
        gu[...] = jnp.zeros_like(gu)
        gd[...] = jnp.zeros_like(gd)

    pre = dot(t[0, 0], up[...], ((1,), (1,)))
    act, gelu_back = jax.vjp(gelu_tanh, pre)
    hidden = act.astype(BF)
    d_pre = gelu_back(dot(t[1, 0], dn[...], ((1,), (1,))))[0].astype(BF)
    cols = width // 4
    for n in range(4):
        at = slice(n * cols, (n + 1) * cols)
        pp[0, 0, :, :, :, at] = dot(hidden, dn[:, at], ((1,), (0,))).astype(BF).reshape(*pp.shape[2:5], cols)
        pp[1, 0, :, :, :, at] = dot(d_pre, up[:, at], ((1,), (0,))).astype(BF).reshape(*pp.shape[2:5], cols)
        gu[:, at] += dot(d_pre, t[0, 0, :, at], ((0,), (0,)))
        gd[:, at] += dot(hidden, t[1, 0, :, at], ((0,), (0,)))

    @pl.when(m == pl.num_programs(0) - 1)
    def _():
        for j in range(pairs):
            u = gu[:, j * lanes : (j + 1) * lanes].astype(BF)
            d = gd[:, j * lanes : (j + 1) * lanes].astype(BF)
            qq[2 * j] = jnp.concatenate([u[:, :part], d[:, :part]], axis=1)
            qq[2 * j + 1] = jnp.concatenate([u[:, part:], d[:, part:]], axis=1)


def mlp(g, t):
    hid, lanes = g.shape[2:]
    n_tok, width = t.shape[2:]
    flops = 12 * 4 * n_tok * width * hid
    return pl.pallas_call(
        mlp_kernel,
        grid=(4,),
        out_shape=(
            jax.ShapeDtypeStruct((2, 4, 2, 4, n_tok // 8, width), BF),
            jax.ShapeDtypeStruct((16, hid, lanes), BF),
        ),
        in_specs=[
            pl.BlockSpec((16, hid, lanes), lambda m: (0, 0, 0)),
            pl.BlockSpec((2, 1, n_tok, width), lambda m: (0, m, 0, 0)),
        ],
        out_specs=(
            pl.BlockSpec((2, 1, 2, 4, n_tok // 8, width), lambda m: (0, m, 0, 0, 0, 0)),
            pl.BlockSpec((16, hid, lanes), lambda m: (0, 0, 0)),
        ),
        scratch_shapes=[
            pltpu.VMEM((hid, width), BF),
            pltpu.VMEM((hid, width), BF),
            pltpu.VMEM((hid, width), F32),
            pltpu.VMEM((hid, width), F32),
        ],
        compiler_params=pltpu.CompilerParams(vmem_limit_bytes=60 * 2**20),
        cost_estimate=pl.CostEstimate(flops=flops, bytes_accessed=30 * 2**20, transcendentals=0),
        name="mlp",
    )(g.reshape(16, hid, lanes), t)


def shards(
    image_tokens, text_tokens, null_prompt, drop_flags, time_index, modulation, w_up, w_down, d_output
):
    dropped = drop_flags == 1
    text_in = jnp.where(dropped[:, None, None], null_prompt[None], text_tokens)[0]
    n_text = text_in.shape[0]

    def blocked(text, image):
        wide = text.shape[-1]
        both = [text.reshape(8, -1, wide), image.reshape(8, -1, wide)]
        return jnp.concatenate(both, axis=1).reshape(-1, wide)

    def in_order(rows):
        wide = rows.shape[-1]
        parts = [rows[:, : n_text // 8], rows[:, n_text // 8 :]]
        return jnp.concatenate([p.reshape(-1, wide) for p in parts], axis=0)[None]

    joined = blocked(text_in, image_tokens[0])
    d_out = blocked(d_output[0, :n_text], d_output[0, n_text:])
    mods = lax.dynamic_index_in_dim(modulation, time_index[0], 0, keepdims=False)
    shift, scale, gate = mods[0:1], mods[1:2], mods[2:3]
    length, width = joined.shape
    joined32 = joined.astype(F32)
    centred = joined32 - jnp.mean(joined32, axis=-1, keepdims=True)
    inv_std = lax.rsqrt(jnp.mean(centred * centred, axis=-1, keepdims=True) + EPS)
    mod_in = (centred * inv_std * (1.0 + scale) + shift).astype(BF)
    d_branch = (d_out.astype(F32) * gate).astype(BF)

    d_part, hid_all = w_up.shape
    hid = hid_all // 4
    pk = jnp.concatenate([w_up.T, w_down], axis=1).reshape(4, hid, 2 * d_part)
    g, t = gather(pk, jnp.stack([mod_in, d_branch]))
    pp, qq = mlp(g, t)
    qq = qq.reshape(4, 4, hid, 2 * d_part)
    flag = jnp.broadcast_to(dropped.astype(F32)[:, None], (1, width))
    ob, gn, gr = reduce_all(pp, qq, joined, d_out, mods, flag)
    grads = gr.reshape(hid_all, 2 * d_part).astype(F32)
    return (
        in_order(ob[0]),
        in_order(ob[1]),
        grads[:, :d_part].T,
        grads[:, d_part:],
        gn.reshape(null_prompt.shape).astype(F32),
    )


def solution(mesh):
    torus = Mesh(mesh.devices.reshape(4, 4, 4, 2, 2), AXES)
    in_specs = (
        P(DP, None, None),
        P(DP, None, None),
        P(),
        P(DP),
        P(DP),
        P(),
        P(DP, MP),
        P(MP, DP),
        P(DP, None, None),
    )
    out_specs = (P(DP, None, None), P(DP, None, None), P(DP, MP), P(MP, DP), P())
    return jax.shard_map(shards, mesh=torus, in_specs=in_specs, out_specs=out_specs, check_vma=False)
```

```python
import jax
import jax.numpy as jnp
from jax import lax
from jax.experimental import pallas as pl
from jax.experimental.pallas import tpu as pltpu
from jax.sharding import Mesh
from jax.sharding import PartitionSpec as P

AXES = ("zl", "y", "x", "zh", "c")
MP = ("x", "zh", "c")
DP = ("zl", "y")
EPS = 1e-06
MESH = pl.DeviceIdType.MESH
BF = jnp.bfloat16
F32 = jnp.float32


def gelu_tanh(values):
    return jax.nn.gelu(values, approximate=True)


def remote(src, dst, ss, rs, **dev):
    return pltpu.make_async_remote_copy(
        src_ref=src, dst_ref=dst, send_sem=ss, recv_sem=rs, device_id=dev, device_id_type=MESH
    )


def meet(devices):
    barrier = pltpu.get_barrier_semaphore()
    for dev in devices:
        pl.semaphore_signal(barrier, inc=1, device_id=dev, device_id_type=MESH)
    pl.semaphore_wait(barrier, len(devices))


def along_z(zl, zh, dist):
    to = lax.rem(zh * 4 + zl + dist % 8, 8)
    return {"zl": lax.rem(to, 4), "zh": to // 4}


def dot(left, right, dims):
    return lax.dot_general(left, right, (dims, ((), ())), preferred_element_type=F32)


def step_kernel(
    pk, jo, do, mods,
    ob, gn, gr,
    t, g, up, dn, PA, HD, pp, qq,
    R, X1, F1, X2, F2, RB, Z, O, FIN, ZR, ZL, YN, ZN, GN, JD,
    lsem, gws0, gwr0, gzs0, gzr0, ys, yr, ps, pr, xs, xr, bs, br,
    cs, cr, e1s, e1r, e2s, e2r, hs, hr, hs2, hr2, zs, zr, ws, wr, ags, agr, ags2, agr2, abs_, abr,
    gys, gyr, gzs, gzr, gxs, gxr, gbs, gbr,
):
    zl, y, x, zh, c = (lax.axis_index(n) for n in AXES)
    meet(
        [{"y": lax.rem(y + d, 4)} for d in (1, 2, 3)]
        + [{"x": lax.rem(x + d, 4)} for d in (1, 2, 3)]
        + [along_z(zl, zh, d) for d in (1, -1, 2, -2, 3, -3)]
        + [{"c": 1 - c}]
    )
    yp, yo, ym = lax.rem(y + 1, 4), lax.rem(y + 2, 4), lax.rem(y + 3, 4)
    xp, xo, xm = lax.rem(x + 1, 4), lax.rem(x + 2, 4), lax.rem(x + 3, 4)
    qrt = jo.shape[0] // 4
    half = qrt // 2
    par = lax.rem(x, 2)
    peers = (ym, yp, yo)
    sent = []

    def rows(quarter, h, n=1):
        return pl.ds(pl.multiple_of(quarter * qrt + h * half, half), n * half)

    own_q = par * 2 + c
    x_q = (1 - par) * 2 + c
    sib_q = (par * 2 + (1 - c), (1 - par) * 2 + (1 - c))

    def w1(d):
        to = lax.rem(y + d, 4)
        return remote(pk.at[to], g.at[zl, y], gws0.at[d - 1], gwr0.at[d - 1], y=to)

    for d in (1, 3, 2):
        w1(d).start()
        sent.append((None, w1(d)))
    pk_own = pltpu.make_async_copy(pk.at[y], g.at[zl, y], lsem.at[0])
    pk_own.start()
    n_r = O.shape[1]
    blk = c * 4 + x
    loads = [pltpu.make_async_copy(r, JD.at[i], lsem.at[3 + i]) for i, r in enumerate((jo, do))]
    for cp in loads:
        cp.start()

    def norm_of(tok):
        cen = tok - jnp.mean(tok, axis=-1, keepdims=True)
        inv = lax.rsqrt(jnp.mean(cen * cen, axis=-1, keepdims=True) + EPS)
        return cen * inv, inv

    def zcopy(way, s, d):
        yd = lax.rem(y + 4 - d, 4)
        block = zl - s if way == 0 else zl + s
        src = pk.at[y] if (s == 0 and d == 0) else g.at[block, yd]
        to = zl + 1 if way == 0 else zl - 1
        return remote(src, g.at[block, yd], gzs0.at[way, s, d], gzr0.at[way, s, d], zl=to)

    def zsend(way, s, d):
        ok = (zl < 3) & (zl >= s) if way == 0 else (zl > 0) & (zl + s <= 3)

        @pl.when(ok)
        def _():
            zcopy(way, s, d).start()

        sent.append((ok, (way, s, d)))

    def gtick(s, d):
        for way in (0, 1):
            got = zl >= s if way == 0 else zl + s <= 3
            yd = lax.rem(y + 4 - d, 4)

            @pl.when(got)
            def _():
                block = zl - s if way == 0 else zl + s
                remote(
                    g.at[block, yd], g.at[block, yd], gzs0.at[way, s - 1, d], gzr0.at[way, s - 1, d], zl=zl
                ).wait_recv()

            if s <= 2:
                zsend(way, s, d)

    def wstep(d):
        if d:
            w1(d).wait_recv()
        for way in (0, 1):
            zsend(way, 0, d)

    wstep(0)

    def send_own(a):
        for way, to in ((0, yp), (1, ym)):
            src = t.at[a, y, rows(own_q, 0, 2)]
            cp = remote(src, src, ys.at[a, way], yr.at[a, way], y=to)
            cp.start()
            sent.append((None, cp))

    def ready(a, first_block, n_blocks):
        def body(i, carry):
            at = lax.rem(own_q * qrt + (first_block + i) * 16, 4 * qrt)
            rr = pl.ds(pl.multiple_of(at, 16), 16)
            val = JD[a, rr, :].astype(F32)
            if a == 0:
                t[0, y, rr, :] = (norm_of(val)[0] * (1.0 + mods[1:2, :]) + mods[0:1, :]).astype(BF)
            else:
                t[1, y, rr, :] = (val * mods[2:3, :]).astype(BF)
            return carry

        lax.fori_loop(0, n_blocks, body, 0)

    for a in range(2):
        loads[a].wait()
        ready(a, 0, qrt // 16)
        send_own(a)
        if a == 0:
            wstep(1)
            wstep(3)
    for a in range(2):
        ready(a, qrt // 16, 3 * qrt // 16)

    def send_on(a, peer, h):
        src = t.at[a, peers[peer], rows(own_q, h)]
        for cp in (
            remote(src, src, xs.at[a, peer, h], xr.at[a, peer, h], x=(xp, xm)[h]),
            remote(src, src, bs.at[a, peer, h], br.at[a, peer, h], c=1 - c),
        ):
            cp.start()
            sent.append((None, cp))

    def direct(a, way):
        whole = t.at[a, peers[way], rows(own_q, 0, 2)]
        remote(whole, whole, ys.at[a, way], yr.at[a, way], y=y).wait_recv()
        part = t.at[a, peers[way], rows(own_q, way)]
        cp = remote(part, part, ps.at[a, way], pr.at[a, way], y=(yp, ym)[way])
        cp.start()
        sent.append((None, cp))
        for h in (0, 1):
            send_on(a, way, h)

    def relayed(a, h):
        part = t.at[a, yo, rows(own_q, h)]
        remote(part, part, ps.at[a, h], pr.at[a, h], y=y).wait_recv()
        send_on(a, 2, h)

    def from_x(a, peer):
        for h in (0, 1):
            part = t.at[a, peers[peer], rows(x_q, h)]
            remote(part, part, xs.at[a, peer, h], xr.at[a, peer, h], x=x).wait_recv()
            cp = remote(part, part, bs.at[a, peer, 2 + h], br.at[a, peer, 2 + h], c=1 - c)
            cp.start()
            sent.append((None, cp))

    gtick(1, 0)
    wstep(2)
    gtick(1, 1)
    direct(0, 1)
    gtick(1, 3)
    gtick(1, 2)
    direct(0, 0)
    gtick(2, 0)
    direct(1, 1)
    gtick(2, 1)
    relayed(0, 1)
    from_x(0, 1)
    direct(1, 0)
    gtick(2, 3)
    from_x(0, 0)
    gtick(2, 2)
    relayed(1, 1)
    relayed(0, 0)
    gtick(3, 0)
    from_x(1, 1)
    relayed(1, 0)
    gtick(3, 1)
    from_x(1, 0)
    from_x(0, 2)
    gtick(3, 3)
    gtick(3, 2)
    from_x(1, 2)
    for a in range(2):
        for peer in range(3):
            for kind in range(4):
                part = t.at[a, peers[peer], rows(sib_q[kind // 2], kind % 2)]
                remote(part, part, bs.at[a, peer, kind], br.at[a, peer, kind], c=c).wait_recv()
    pk_own.wait()

    first = c == 0
    p1 = jnp.where(first, y, x)
    p2 = jnp.where(first, x, y)
    width = pp.shape[5]
    step_r = 16
    blocks = n_r // step_r

    flying = {}

    def start(cp, key=None):
        cp.start()
        flying[key if key is not None else len(flying) + 1000] = cp

    def drain(*key):
        for w in (0, 1):
            flying.pop((*key, w)).wait_send()

    def nb(stage, sign):
        s = sign % 4
        along_y = first if stage == 1 else c == 1
        return {
            "y": jnp.where(along_y, lax.rem(y + s, 4), y),
            "x": jnp.where(along_y, x, lax.rem(x + s, 4)),
        }

    def zblock(way, k, h, from_input):
        buf = ZR if way == 0 else ZL
        at = pl.ds(2 * h, 2)
        src = qq.at[k, at] if from_input else buf.at[k, at]
        to = zl + 1 if way == 0 else zl - 1
        return remote(src, buf.at[k, at], zs.at[way, k, h], zr.at[way, k, h], zl=to)

    hid = qq.shape[2]
    q_rows = 48

    def q_at(i):
        return i // (hid // q_rows), pl.ds(pl.multiple_of(lax.rem(i, hid // q_rows) * q_rows, 16), q_rows)

    def z_end(n, ways=(0, 1)):
        for way in ways:
            k = 3 - n if way == 0 else n

            @pl.when(zl == 3 * way)
            def _():
                for h in (0, 1):
                    zblock(way, k, h, True).start()

    def z_mid(way, k, who, h):
        buf = ZR if way == 0 else ZL

        @pl.when(zl == who)
        def _():
            zblock(way, k, h, False).wait_recv()

            def body(i, carry):
                p, r = q_at(i)
                p = p + 2 * h
                buf[k, p, r, :] = (buf[k, p, r, :].astype(F32) + qq[k, p, r, :].astype(F32)).astype(BF)
                return carry

            lax.fori_loop(0, 2 * hid // q_rows, body, 0)
            zblock(way, k, h, False).start()

    def own_sum(a, d):
        k = lax.rem(p1 + d, 4)
        remote(R.at[a, k], R.at[a, k], cs.at[a, d], cr.at[a, d], c=c).wait_recv()

        def body(n, carry):
            j, r = n // blocks, lax.rem(n, blocks)
            iy, ix = jnp.where(first, k, j), jnp.where(first, j, k)
            rr = pl.ds(pl.multiple_of(r * step_r, step_r), step_r)
            R[a, k, j, rr, :] = (
                R[a, k, j, rr, :].astype(F32) + pp[a, iy, c, ix, rr, :].astype(F32)
            ).astype(BF)
            return carry

        lax.fori_loop(0, 4 * blocks, body, 0)

    hr_n = n_r // 2

    def half_rows(way):
        return pl.ds(way * hr_n, hr_n)

    def view(stage, a, w, d):
        if stage == 1:
            return R.at[a, lax.rem(p1 + d, 4), :, half_rows(w)]
        return R.at[a, p1, lax.rem(p2 + d, 4), half_rows(w)]

    def bufs(stage):
        return (X1, F1, e1s, e1r) if stage == 1 else (X2, F2, e2s, e2r)

    def add_to(stage, a, w, d, *srcs):
        if stage == 1:
            k = lax.rem(p1 + d, 4)

            def body(j, carry):
                total = R[a, k, j, half_rows(w), :].astype(F32)
                for s in srcs:
                    total = total + s[j].astype(F32)
                R[a, k, j, half_rows(w), :] = total.astype(BF)
                return carry

            lax.fori_loop(0, 4, body, 0)
        else:
            k = lax.rem(p2 + d, 4)
            total = R[a, p1, k, half_rows(w), :].astype(F32)
            for s in srcs:
                total = total + s[...].astype(F32)
            R[a, p1, k, half_rows(w), :] = total.astype(BF)

    def ring_first(stage, a):
        X, F, es, er = bufs(stage)
        for w, sg in ((0, 1), (1, -1)):
            start(
                remote(view(stage, a, w, 2), X.at[a, w], es.at[a, w, 0], er.at[a, w, 0], **nb(stage, sg)),
                (stage, a, 0, w),
            )

    def ring_own(stage, a, w):
        X, F, es, er = bufs(stage)
        sg = (1, -1)[w]
        src = view(stage, a, w, -sg % 4)
        start(
            remote(src, F.at[1, a, w], es.at[a, w, 1], er.at[a, w, 1], **nb(stage, -sg)), (stage, a, 1, w)
        )

    def ring_pass(stage, a):
        X, F, es, er = bufs(stage)
        for w, sg in ((0, 1), (1, -1)):
            remote(X.at[a, w], X.at[a, w], es.at[a, w, 0], er.at[a, w, 0], c=c).wait_recv()
            add_to(stage, a, w, sg % 4, X.at[a, w])
            src = view(stage, a, w, sg % 4)
            start(
                remote(src, F.at[0, a, w], es.at[a, w, 2], er.at[a, w, 2], **nb(stage, sg)),
                (stage, a, 2, w),
            )

    def ring_last(stage, a, w):
        X, F, es, er = bufs(stage)
        remote(F.at[1, a, w], F.at[1, a, w], es.at[a, w, 1], er.at[a, w, 1], c=c).wait_recv()
        remote(F.at[0, a, w], F.at[0, a, w], es.at[a, w, 2], er.at[a, w, 2], c=c).wait_recv()
        add_to(stage, a, w, 0, F.at[0, a, w], F.at[1, a, w])

    def zh_send(a, way):
        mine = R.at[a, p1, p2, half_rows(way)]
        return remote(mine, RB.at[a, way], hs.at[a, way], hr.at[a, way], **along_z(zl, zh, (1, -1)[way]))

    def zh_pass(a):
        for way in (0, 1):
            remote(RB.at[a, way], RB.at[a, way], hs.at[a, way], hr.at[a, way], c=c).wait_recv()
            start(
                remote(
                    RB.at[a, way],
                    Z.at[a, half_rows(way)],
                    hs2.at[a, way],
                    hr2.at[a, way],
                    **along_z(zl, zh, (3, -3)[way]),
                )
            )

    def stage_two(a):
        for w in (0, 1):
            ring_last(1, a, w)
        ring_first(2, a)
        for w in (0, 1):
            ring_own(2, a, w)

    def stage_zh(a):
        for w in (0, 1):
            ring_last(2, a, w)
            start(zh_send(a, w))

    lanes = g.shape[3]
    part = lanes // 2
    n_tok = t.shape[2]
    for j in range(8):
        at = slice(j * lanes, (j + 1) * lanes)
        one, two = g.at[2 * j // 4, 2 * j % 4], g.at[(2 * j + 1) // 4, (2 * j + 1) % 4]
        up[:, at] = jnp.concatenate([one[:, :part], two[:, :part]], axis=1)
        dn[:, at] = jnp.concatenate([one[:, part:], two[:, part:]], axis=1)

    def tok_rows(s):
        return pl.ds(pl.multiple_of(s * n_tok, n_tok), n_tok)

    PA[0] = dot(t[0].reshape(4 * n_tok, width), up[...], ((1,), (1,)))
    PA[1] = dot(t[1].reshape(4 * n_tok, width), dn[...], ((1,), (1,)))

    def hidden_of(i, carry):
        rr = pl.ds(pl.multiple_of(i * 64, 64), 64)
        act, gelu_back = jax.vjp(gelu_tanh, PA[0, rr, :])
        HD[0, rr, :] = act.astype(BF)
        HD[1, rr, :] = gelu_back(PA[1, rr, :])[0].astype(BF)
        return carry

    lax.fori_loop(0, 4 * n_tok // 64, hidden_of, 0)

    def weight_grads(k):
        at = slice(2 * k * lanes, 2 * (k + 1) * lanes)
        u = dot(HD[1], t[0, :, :, at].reshape(4 * n_tok, 2 * lanes), ((0,), (0,))).astype(BF)
        v = dot(HD[0], t[1, :, :, at].reshape(4 * n_tok, 2 * lanes), ((0,), (0,))).astype(BF)
        for p in range(4):
            cut = slice(p * part, (p + 1) * part)
            qq[k, p] = jnp.concatenate([u[:, cut], v[:, cut]], axis=1)

    o_first = c == 1
    op1 = jnp.where(o_first, y, x)

    def token_grads(a):
        weights, kept = (dn, up)[a], HD.at[a]

        def sample(i, carry):
            s = lax.rem(y + jnp.where(i == 0, 2, jnp.where(i == 1, 1, jnp.where(i == 2, 3, 0))), 4)
            cols = width // 4
            for n in range(4):
                at = slice(n * cols, (n + 1) * cols)
                out = dot(kept[tok_rows(s), :], weights[:, at], ((1,), (0,)))
                pp[a, s, :, :, :, at] = out.astype(BF).reshape(2, 4, n_r, cols)
            for xx in range(4):
                k, j = jnp.where(o_first, s, xx), jnp.where(o_first, xx, s)
                d = lax.rem(k + 4 - op1, 4)
                remote(pp.at[a, s, 1 - c, xx], R.at[a, k, j], cs.at[a, d], cr.at[a, d], c=1 - c).start()
            return carry

        lax.fori_loop(0, 4, sample, 0)

    weight_grads(3)
    z_end(0, (0,))
    weight_grads(0)
    z_end(0, (1,))
    weight_grads(2)
    weight_grads(1)
    token_grads(1)
    own_sum(1, 2)
    ring_first(1, 1)
    own_sum(1, 3)
    own_sum(1, 1)
    own_sum(1, 0)
    token_grads(0)
    z_end(1)
    drain(1, 1, 0)
    ring_own(1, 1, 0)
    ring_own(1, 1, 1)
    own_sum(0, 2)
    ring_pass(1, 1)
    own_sum(0, 3)
    own_sum(0, 1)
    own_sum(0, 0)
    drain(1, 1, 1)
    ring_first(1, 0)
    for h in (0, 1):
        z_mid(0, 3, 1, h)
        z_mid(1, 0, 2, h)
    stage_two(1)
    z_end(2)
    drain(1, 0, 0)
    ring_own(1, 0, 0)
    ring_own(1, 0, 1)
    ring_pass(1, 0)
    for h in (0, 1):
        z_mid(0, 2, 1, h)
        z_mid(1, 1, 2, h)
    ring_pass(2, 1)
    stage_zh(1)
    for h in (0, 1):
        z_mid(0, 3, 2, h)
        z_mid(1, 0, 1, h)
    zh_pass(1)
    stage_two(0)
    ring_pass(2, 0)
    stage_zh(0)

    def wcopy(d):
        to = lax.rem(y + d, 4)
        return remote(FIN.at[to], gr.at[y], ws.at[d], wr.at[d], y=to)

    def grad_final(d):
        p = lax.rem(y + d, 4)

        def body(i, carry):
            r = pl.ds(pl.multiple_of(i * 48, 16), 48)
            zero = jnp.zeros((48, qq.shape[3]), F32)
            total = qq[zl, p, r, :].astype(F32)
            total = total + jnp.where(zl > 0, ZR[zl, p, r, :].astype(F32), zero)
            total = total + jnp.where(zl < 3, ZL[zl, p, r, :].astype(F32), zero)
            FIN[p, r, :] = total.astype(BF)
            return carry

        lax.fori_loop(0, hid // 48, body, 0)
        if d:
            start(wcopy(d))

    n_text = YN.shape[1]

    def rows_done(a):
        for way in (0, 1):
            part = Z.at[a, half_rows(way)]
            remote(part, part, hs2.at[a, way], hr2.at[a, way], c=c).wait_recv()

        def body(r, carry):
            rr = pl.ds(pl.multiple_of(r * 16, 16), 16)
            total = R[a, p1, p2, rr, :].astype(F32) + Z[a, rr, :].astype(F32)
            at = pl.ds(pl.multiple_of(blk * n_r + r * 16, 16), 16)
            tok = JD[0, at, :].astype(F32)
            if a == 0:
                O[0, rr, :] = (tok + mods[2:3, :] * total).astype(BF)
            else:
                normed, inv = norm_of(tok)
                dn = total * (1.0 + mods[1:2, :])
                full = JD[1, at, :].astype(F32) + inv * (
                    dn
                    - jnp.mean(dn, axis=-1, keepdims=True)
                    - normed * jnp.mean(dn * normed, axis=-1, keepdims=True)
                )
                O[1, rr, :] = full.astype(BF)

                @pl.when(r == 0)
                def _():
                    YN[y] = jnp.where(mods[3:4, :] > 0.5, full[:n_text], 0.0).astype(BF)

            return carry

        lax.fori_loop(0, n_r // 16, body, 0)

    locs = []

    def gather_start(a):
        for way, to in ((0, xp), (1, xm)):
            start(remote(O.at[a], ob.at[a, blk], ags.at[a, way], agr.at[a, way], x=to))
        start(remote(O.at[a], ob.at[a, blk], abs_.at[a, 0], abr.at[a, 0], c=1 - c))
        cp = pltpu.make_async_copy(O.at[a], ob.at[a, blk], lsem.at[1 + a])
        cp.start()
        locs.append(cp)

    def gather_near(a):
        for way, frm in ((0, xm), (1, xp)):
            part = ob.at[a, c * 4 + frm]
            remote(part, part, ags.at[a, way], agr.at[a, way], x=x).wait_recv()
            piece = ob.at[a, c * 4 + frm, half_rows(way)]
            start(remote(piece, piece, ags2.at[a, way], agr2.at[a, way], x=(xp, xm)[way]))
            start(remote(part, part, abs_.at[a, 1 + way], abr.at[a, 1 + way], c=1 - c))

    def gather_far(a):
        for way in (0, 1):
            piece = ob.at[a, c * 4 + xo, half_rows(way)]
            remote(piece, piece, ags2.at[a, way], agr2.at[a, way], x=x).wait_recv()
            start(remote(piece, piece, abs_.at[a, 3 + way], abr.at[a, 3 + way], c=1 - c))

    def gy(d):
        return remote(YN.at[y], YN.at[y], gys.at[d], gyr.at[d], y=lax.rem(y + d, 4))

    def gz(d):
        return remote(ZN.at[zl], ZN.at[zl], gzs.at[d], gzr.at[d], zl=lax.rem(zl + d, 4))

    def gx(d):
        return remote(GN, gn.at[blk], gxs.at[d], gxr.at[d], x=lax.rem(x + d, 4))

    def sum_slots(src, dst):
        total = src[0].astype(F32)
        for i in range(1, 4):
            total = total + src[i].astype(F32)
        dst[...] = total.astype(BF)

    def got(buf, me, sems, semr):
        for d in (1, 3, 2):
            slot = buf.at[lax.rem(me + 4 - d, 4)]
            remote(slot, slot, sems.at[d], semr.at[d], c=c).wait_recv()

    rows_done(1)
    for d in (2, 1, 3):
        start(gy(d))
    gather_start(1)
    zh_pass(0)
    got(YN, y, gys, gyr)
    sum_slots(YN, ZN.at[zl])
    for d in (1, 2, 3):
        start(gz(d))
    gather_near(1)
    rows_done(0)
    gather_start(0)
    for way in (0, 1):

        @pl.when(zl != 3 * way)
        def _():
            for h in (0, 1):
                zblock(way, zl, h, False).wait_recv()

    for d in (2, 1, 3, 0):
        grad_final(d)
    loc_gr = pltpu.make_async_copy(FIN.at[y], gr.at[y], lsem.at[0])
    loc_gr.start()
    locs.append(loc_gr)
    got(ZN, zl, gzs, gzr)
    sum_slots(ZN, GN)
    for d in (2, 1, 3):
        start(gx(d))
    start(remote(GN, gn.at[blk], gbs.at[0], gbr.at[0], c=1 - c))
    loc_gn = pltpu.make_async_copy(GN, gn.at[blk], lsem.at[3])
    loc_gn.start()
    locs.append(loc_gn)
    gather_far(1)
    gather_near(0)
    for d in (1, 3, 2):
        part = gn.at[c * 4 + lax.rem(x + 4 - d, 4)]
        remote(part, part, gxs.at[d], gxr.at[d], x=x).wait_recv()
        start(remote(part, part, gbs.at[d], gbr.at[d], c=1 - c))
    gather_far(0)
    for d in range(4):
        part = gn.at[(1 - c) * 4 + lax.rem(x + 4 - d, 4)]
        remote(part, part, gbs.at[d], gbr.at[d], c=c).wait_recv()

    for a in range(2):
        for i, frm in enumerate((x, xm, xp, xo, xo)):
            part = ob.at[a, (1 - c) * 4 + frm]
            if i >= 3:
                part = ob.at[a, (1 - c) * 4 + frm, half_rows(i - 3)]
            remote(part, part, abs_.at[a, i], abr.at[a, i], c=c).wait_recv()
    for d in (1, 2, 3):
        frm = gr.at[lax.rem(y + 4 - d, 4)]
        remote(frm, frm, ws.at[d], wr.at[d], y=y).wait_recv()
    for cp in locs:
        cp.wait()
    for cp in flying.values():
        cp.wait_send()
    for d in (2, 1, 3, 0):
        for a in range(2):
            remote(R.at[a, 0], R.at[a, 0], cs.at[a, d], cr.at[a, d], c=1 - c).wait_send()
    for way in (0, 1):
        for k in range(4):

            @pl.when(zl < k if way == 0 else zl > k)
            def _():
                for h in (0, 1):
                    zblock(way, k, h, False).wait_send()

    for ok, cp in sent:
        if ok is None:
            cp.wait_send()
        else:
            way, s, d = cp

            @pl.when(ok)
            def _():
                zcopy(way, s, d).wait_send()


def step(pk, jo, do, mods):
    n_tok, width = jo.shape
    hid, lanes = pk.shape[1:]
    n_r = n_tok // 8
    half, eighth = n_r // 2, n_r // 4
    vm = pl.BlockSpec(memory_space=pltpu.VMEM)
    hbm = pl.BlockSpec(memory_space=pl.ANY)

    def buf(*shape):
        return pltpu.VMEM(shape, BF)

    counts = [(5,), (3,), (3,), (2, 3, 4), (2, 3, 4), (2, 2), (2, 2), (2, 2), (2, 2)]
    counts += [(2, 3, 2), (2, 3, 2), (2, 3, 4), (2, 3, 4)]
    counts += [(2, 4)] * 2 + [(2, 2, 3)] * 4 + [(2, 2)] * 4 + [(2, 4, 2)] * 2 + [(4,)] * 2
    counts += [(2, 2)] * 4 + [(2, 5)] * 2 + [(4,)] * 8
    return pl.pallas_call(
        step_kernel,
        out_shape=(
            jax.ShapeDtypeStruct((2, 8, n_r, width), BF),
            jax.ShapeDtypeStruct((8, eighth, width), BF),
            jax.ShapeDtypeStruct((4, hid, lanes), BF),
        ),
        in_specs=[vm, hbm, hbm, vm],
        out_specs=(hbm,) * 3,
        scratch_shapes=[
            buf(2, 4, n_tok, width),
            buf(4, 4, hid, lanes),
            buf(hid, width),
            buf(hid, width),
            pltpu.VMEM((2, 4 * n_tok, hid), F32),
            buf(2, 4 * n_tok, hid),
            buf(2, 4, 2, 4, n_r, width),
            buf(4, 4, hid, lanes),
            buf(2, 4, 4, n_r, width),
            buf(2, 2, 4, half, width),
            buf(2, 2, 2, 4, half, width),
            buf(2, 2, half, width),
            buf(2, 2, 2, half, width),
            buf(2, 2, half, width),
            buf(2, n_r, width),
            buf(2, n_r, width),
            buf(4, hid, lanes),
            buf(4, 4, hid, lanes),
            buf(4, 4, hid, lanes),
            buf(4, eighth, width),
            buf(4, eighth, width),
            buf(eighth, width),
            buf(2, n_tok, width),
        ]
        + [pltpu.SemaphoreType.DMA(n) for n in counts],
        compiler_params=pltpu.CompilerParams(
            collective_id=1, has_side_effects=True, vmem_limit_bytes=67043328
        ),
        name="step",
    )(pk, jo, do, mods)


def shards(
    image_tokens, text_tokens, null_prompt, drop_flags, time_index, modulation, w_up, w_down, d_output
):
    dropped = drop_flags == 1
    text_in = jnp.where(dropped[:, None, None], null_prompt[None], text_tokens)[0]
    n_text = text_in.shape[0]

    def blocked(text, image):
        wide = text.shape[-1]
        both = [text.reshape(8, -1, wide), image.reshape(8, -1, wide)]
        return jnp.concatenate(both, axis=1).reshape(-1, wide)

    def in_order(rows):
        wide = rows.shape[-1]
        parts = [rows[:, : n_text // 8], rows[:, n_text // 8 :]]
        return jnp.concatenate([p.reshape(-1, wide) for p in parts], axis=0)[None]

    joined = blocked(text_in, image_tokens[0])
    d_out = blocked(d_output[0, :n_text], d_output[0, n_text:])
    width = joined.shape[-1]
    mods = lax.dynamic_index_in_dim(modulation, time_index[0], 0, keepdims=False)
    mods = jnp.concatenate([mods, jnp.broadcast_to(dropped.astype(F32)[:, None], (1, width))], axis=0)

    d_part, hid_all = w_up.shape
    hid = hid_all // 4
    pk = jnp.concatenate([w_up.T, w_down], axis=1).reshape(4, hid, 2 * d_part)
    ob, gn, gr = step(pk, joined, d_out, mods)
    grads = gr.reshape(hid_all, 2 * d_part).astype(F32)
    return (
        in_order(ob[0]),
        in_order(ob[1]),
        grads[:, :d_part].T,
        grads[:, d_part:],
        gn.reshape(null_prompt.shape).astype(F32),
    )


def solution(mesh):
    torus = Mesh(mesh.devices.reshape(4, 4, 4, 2, 2), AXES)
    in_specs = (
        P(DP, None, None),
        P(DP, None, None),
        P(),
        P(DP),
        P(DP),
        P(),
        P(DP, MP),
        P(MP, DP),
        P(DP, None, None),
    )
    out_specs = (P(DP, None, None), P(DP, None, None), P(DP, MP), P(MP, DP), P())
    return jax.shard_map(shards, mesh=torus, in_specs=in_specs, out_specs=out_specs, check_vma=False)
```
